128 devices in a mesh: stage: 1, model: 64 (over z, y, x), data: 2 (over core).
Axes of the slice: x: 4, y: 4, z: 4, core: 2. Of those that a mesh axis runs over, the one named last changes fastest.
Arguments:
- w_fc1: float32 [4, 1024, 1024], P('stage', 'data', 'model')
- m_fc1: float32 [4, 1024, 1024], P('stage', 'data', 'model')
- g_fc1: bfloat16 [4, 1024, 1024], P('stage', 'data', 'model')
- w_fc2: float32 [4, 1024, 512], P('stage', 'data', 'model')
- m_fc2: float32 [4, 1024, 512], P('stage', 'data', 'model')
- g_fc2: bfloat16 [4, 1024, 512], P('stage', 'data', 'model')
Outputs:
- output 1: float32 [4, 1024, 1024], P('stage', 'data', 'model')
- output 2: float32 [4, 1024, 1024], P('stage', 'data', 'model')
- output 3: float32 [4, 1024, 512], P('stage', 'data', 'model')
- output 4: float32 [4, 1024, 512], P('stage', 'data', 'model')
All inputs are finite; a program needn't handle non-finite values.
Results may differ from the reference program's by a relative error of at most 0.00735249.
Values are sent between devices in bfloat16 or wider.
A program may use at most 1 GiB of HBM per device.

```python
import math
import jax
import jax.numpy as jnp
from jax import lax

HIDDEN = 1024
EXPERT_FFN = 512
EXPERTS = 4
NS_STEPS = 5
LOW_RANK = 4

NS_COEF_A = 3.4445
NS_COEF_B = -4.7750
NS_COEF_C = 2.0315
MOMENTUM = 0.95
LEARN_RATE = 0.04
DECAY = 0.2
NORM_EPS = 1e-7


def draw_state(key, cols):
    key_noise, key_left, key_right, key_scale = jax.random.split(key, 4)
    noise = jax.random.normal(key_noise, (EXPERTS, HIDDEN, cols), jnp.float32)
    left = jax.random.normal(key_left, (EXPERTS, HIDDEN, LOW_RANK), jnp.float32)
    right = jax.random.normal(key_right, (EXPERTS, LOW_RANK, cols), jnp.float32)
    shared = jnp.einsum('emr,ern->emn', left, right) / math.sqrt(LOW_RANK)
    row_scale = jax.random.uniform(key_scale, (EXPERTS, HIDDEN, 1), jnp.float32, 0.5, 1.5)
    return row_scale * (noise + shared) * math.sqrt(0.5)


def setup_inputs(seed: int = 0, part: int = 0) -> dict:
    base = jax.random.fold_in(jax.random.key(seed), part)
    keys = jax.random.split(base, 6)
    fc1_cols = 2 * EXPERT_FFN
    w_scale = HIDDEN ** -0.5
    return {
        'w_fc1': jax.random.normal(keys[0], (EXPERTS, HIDDEN, fc1_cols), jnp.float32) * w_scale,
        'm_fc1': draw_state(keys[1], fc1_cols),
        'g_fc1': draw_state(keys[2], fc1_cols).astype(jnp.bfloat16),
        'w_fc2': jax.random.normal(keys[3], (EXPERTS, HIDDEN, EXPERT_FFN), jnp.float32) * w_scale,
        'm_fc2': draw_state(keys[4], EXPERT_FFN),
        'g_fc2': draw_state(keys[5], EXPERT_FFN).astype(jnp.bfloat16),
    }


def orthogonalize(momentum):
    row_count, col_count = momentum.shape
    norm_val = jnp.sqrt(jnp.sum(momentum * momentum))
    x_mat = (momentum.astype(jnp.bfloat16).astype(jnp.float32) / (norm_val + NORM_EPS)).astype(jnp.bfloat16)
    if row_count > col_count:
        x_mat = x_mat.T
    for ns_step in range(NS_STEPS):
        gram_mat = jnp.dot(x_mat, x_mat.T, preferred_element_type=jnp.float32).astype(jnp.bfloat16)
        gram_sq = jnp.dot(gram_mat, gram_mat, preferred_element_type=jnp.float32)
        poly_mat = (NS_COEF_B * gram_mat.astype(jnp.float32) + NS_COEF_C * gram_sq).astype(jnp.bfloat16)
        update_term = jnp.dot(poly_mat, x_mat, preferred_element_type=jnp.float32)
        x_mat = (NS_COEF_A * x_mat.astype(jnp.float32) + update_term).astype(jnp.bfloat16)
    if row_count > col_count:
        x_mat = x_mat.T
    return x_mat.astype(jnp.float32) * (0.2 * math.sqrt(max(row_count, col_count)))


def update_stack(weights, momentum, gradient):
    new_mom = MOMENTUM * momentum + gradient.astype(jnp.float32)
    ortho = lax.map(orthogonalize, new_mom)
    new_w = weights - LEARN_RATE * (ortho + DECAY * weights)
    return new_w, new_mom


def reference(w_fc1, m_fc1, g_fc1, w_fc2, m_fc2, g_fc2):
    new_w1, new_m1 = update_stack(w_fc1, m_fc1, g_fc1)
    new_w2, new_m2 = update_stack(w_fc2, m_fc2, g_fc2)
    return (new_w1, new_m1, new_w2, new_m2)
```

```python
import math
import jax
import jax.numpy as jnp
from jax import lax
from jax.experimental import pallas as pl
from jax.experimental.pallas import tpu as pltpu
from jax.sharding import PartitionSpec as P

NS_STEPS = 5
NS_COEF_A = 3.4445
NS_COEF_B = -4.7750
NS_COEF_C = 2.0315
MOMENTUM = 0.95
LEARN_RATE = 0.04
DECAY = 0.2
NORM_EPS = 1e-7
F32 = jnp.float32
BF16 = jnp.bfloat16
RING = 4
EXPERTS = 4
ROWS = 512
C1, C2 = 16, 8
N1, N2 = 1024, 512
STEP_SCALE = 0.2 * math.sqrt(1024)


def dot(lhs, rhs, lhs_dim, rhs_dim):
    return lax.dot_general(lhs, rhs, (((lhs_dim,), (rhs_dim,)), ((), ())), preferred_element_type=F32)


def fold(sq):
    total = None
    for row in range(0, sq.shape[0], 8):
        for col in range(0, sq.shape[1], 128):
            tile = sq[row:row + 8, col:col + 128]
            total = tile if total is None else total + tile
    return total


def kernel(m1, g1, m2, g2, w1, w2, nw1, nm1, nw2, nm2,
           mb1, mb2, nb, nz, nx, ny, sx, sy, gat1, gat2,
           ya, yb, aa, ab, ra, rb, b1, y2a, y2b, a2, b2, xo1, xo2, o1, o2, send_sem, recv_sem):
    idx = lax.axis_index('model')
    core = lax.axis_index('data')
    z = lax.div(idx, 16)
    y = lax.rem(lax.div(idx, 4), 4)
    x = lax.rem(idx, 4)

    def at(dz, dy, dx, dc):
        tz, ty, tx = lax.rem(z + dz, RING), lax.rem(y + dy, RING), lax.rem(x + dx, RING)
        return {'model': tz * 16 + ty * 4 + tx, 'data': core if dc == 0 else 1 - core}

    count = [0]
    sent = []

    def put(src, dst, target):
        num = count[0]
        count[0] += 1
        copy = pltpu.make_async_remote_copy(
            src_ref=src, dst_ref=dst, send_sem=send_sem.at[num], recv_sem=recv_sem.at[num],
            device_id=target, device_id_type=pl.DeviceIdType.MESH)
        copy.start()
        sent.append(copy)
        return copy

    def flush():
        while sent:
            sent.pop(0).wait_send()

    z_peers = [(dz, dc) for dz in range(RING) for dc in range(2) if (dz, dc) != (0, 0)]
    barrier = pltpu.get_barrier_semaphore()
    for dz, dc in z_peers:
        pl.semaphore_signal(barrier, inc=1, device_id=at(dz, 0, 0, dc), device_id_type=pl.DeviceIdType.MESH)
    for k in range(1, RING):
        pl.semaphore_signal(barrier, inc=1, device_id=at(0, 0, k, 0), device_id_type=pl.DeviceIdType.MESH)
        pl.semaphore_signal(barrier, inc=1, device_id=at(0, k, 0, 0), device_id_type=pl.DeviceIdType.MESH)

    for e in range(EXPERTS):
        mom = MOMENTUM * m1[e] + g1[e].astype(F32)
        nm1[e] = mom
        mb1[e] = mom.astype(BF16)
        nb[e, 0] = fold(mom * mom)
        mom = MOMENTUM * m2[e] + g2[e].astype(F32)
        nm2[e] = mom
        mb2[e] = mom.astype(BF16)
        nb[e, 1] = fold(mom * mom)
    pl.semaphore_wait(barrier, len(z_peers) + 2 * (RING - 1))

    norm_z = []
    for dz, dc in z_peers:
        norm_z.append(put(nb.at[lax.rem(z + dz, RING)], nz.at[dc, (RING - dz) % RING], at(dz, 0, 0, dc)))
    data_z = [put(mb1.at[lax.rem(z + k, RING)], gat1.at[0, 0, RING - k], at(k, 0, 0, 0)) for k in range(1, RING)]
    data_z2 = [put(mb2.at[lax.rem(z + k, RING)], gat2.at[0, 0, RING - k], at(k, 0, 0, 0)) for k in range(1, RING)]
    gat1[0, 0, 0] = mb1[z]
    gat2[0, 0, 0] = mb2[z]
    for copy in norm_z:
        copy.wait_recv()
    part = nb[z]
    for dz, dc in z_peers:
        part = part + nz[dc, dz]
    sx[...] = part
    norm_x = [put(sx, nx.at[RING - k], at(0, 0, k, 0)) for k in range(1, RING)]

    for copy in data_z:
        copy.wait_recv()
    xp, xm, yp, ym = at(0, 0, 1, 0), at(0, 0, 3, 0), at(0, 1, 0, 0), at(0, 3, 0, 0)
    half_a, half_b = pl.ds(0, 2), pl.ds(2, 2)
    own = gat1.at[0, 0]
    t0 = [put(own, gat1.at[0, 3], xp), put(own, gat1.at[0, 1], xm),
          put(own, gat1.at[3, 0], yp), put(own, gat1.at[1, 0], ym)]

    for copy in norm_x:
        copy.wait_recv()
    part = sx[...]
    for k in range(1, RING):
        part = part + nx[k]
    sy[...] = part
    norm_y = [put(sy, ny.at[RING - k], at(0, k, 0, 0)) for k in range(1, RING)]

    def quarter(dy, dx, q, ty, tx, target):
        return put(gat1.at[dy, dx, q], gat1.at[ty, tx, q], target)

    t1a, t1b = [], []
    t0[0].wait_recv()
    t1a += [put(gat1.at[0, 3, half_a], gat1.at[3, 3, half_a], yp), put(gat1.at[0, 3, half_a], gat1.at[1, 3, half_a], ym)]
    t1b += [quarter(0, 3, 0, 0, 2, xp), quarter(0, 3, 2, 0, 2, xp)]
    t0[1].wait_recv()
    t1a += [put(gat1.at[0, 1, half_a], gat1.at[3, 1, half_a], yp), put(gat1.at[0, 1, half_a], gat1.at[1, 1, half_a], ym)]
    t1b += [quarter(0, 1, 1, 0, 2, xm), quarter(0, 1, 3, 0, 2, xm)]
    t0[2].wait_recv()
    t1a += [put(gat1.at[3, 0, half_b], gat1.at[3, 3, half_b], xp), put(gat1.at[3, 0, half_b], gat1.at[3, 1, half_b], xm)]
    t1b += [quarter(3, 0, 0, 2, 0, yp), quarter(3, 0, 2, 2, 0, yp)]
    t0[3].wait_recv()
    t1a += [put(gat1.at[1, 0, half_b], gat1.at[1, 3, half_b], xp), put(gat1.at[1, 0, half_b], gat1.at[1, 1, half_b], xm)]
    t1b += [quarter(1, 0, 1, 2, 0, ym), quarter(1, 0, 3, 2, 0, ym)]

    for copy in t1b:
        copy.wait_recv()
    t2a = [put(gat1.at[0, 2, half_a], gat1.at[3, 2, half_a], yp), put(gat1.at[0, 2, half_a], gat1.at[1, 2, half_a], ym),
           put(gat1.at[2, 0, half_b], gat1.at[2, 3, half_b], xp), put(gat1.at[2, 0, half_b], gat1.at[2, 1, half_b], xm)]
    for copy in t1a:
        copy.wait_recv()
    t2b = [quarter(3, 3, 0, 2, 3, yp), quarter(3, 1, 0, 2, 1, yp), quarter(1, 3, 1, 2, 3, ym), quarter(1, 1, 1, 2, 1, ym),
           quarter(3, 3, 2, 3, 2, xp), quarter(1, 3, 2, 1, 2, xp), quarter(3, 1, 3, 3, 2, xm), quarter(1, 1, 3, 1, 2, xm)]
    for copy in t2a:
        copy.wait_recv()
    t3 = [quarter(3, 2, 0, 2, 2, yp), quarter(1, 2, 1, 2, 2, ym), quarter(2, 3, 2, 2, 2, xp), quarter(2, 1, 3, 2, 2, xm)]

    for copy in data_z2:
        copy.wait_recv()
    x2 = [put(gat2.at[0, 0], gat2.at[0, RING - k], at(0, 0, k, 0)) for k in range(1, RING)]

    for copy in norm_y:
        copy.wait_recv()
    part = sy[...]
    for k in range(1, RING):
        part = part + ny[k]
    inv1 = 1.0 / (jnp.sqrt(jnp.sum(part[0], keepdims=True)) + NORM_EPS)
    inv2 = 1.0 / (jnp.sqrt(jnp.sum(part[1], keepdims=True)) + NORM_EPS)

    for copy in t2b + t3:
        copy.wait_recv()
    partner = at(0, 0, 0, 1)

    arrive = []
    for c in range(4):
        rows = pl.ds(256 * c, 256)
        ya[rows, 0:ROWS] = (gat1[c].reshape(256, ROWS).astype(F32) * inv1).astype(BF16)
        arrive.append(put(ya.at[rows, pl.ds(0, ROWS)], ya.at[rows, pl.ds(ROWS, ROWS)], partner))

    for copy in x2:
        copy.wait_recv()
    y2p = put(gat2.at[0], gat2.at[3], yp)
    y2m = put(gat2.at[0], gat2.at[1], ym)

    arrive2 = []
    for step in range(NS_STEPS):
        last = step == NS_STEPS - 1
        cur, nxt = (ya, yb) if step % 2 == 0 else (yb, ya)
        gram, panel = (aa, ra) if step % 2 == 0 else (ab, rb)
        gram[0:ROWS, :] = dot(cur[:, 0:ROWS], cur[:, 0:ROWS], 0, 0).astype(BF16)
        swap = put(gram.at[pl.ds(0, ROWS)], panel.at[:, pl.ds(ROWS, ROWS)], partner)
        for copy in arrive:
            copy.wait_recv()
        cross = dot(cur[:, ROWS:], cur[:, 0:ROWS], 0, 0).astype(BF16)
        gram[ROWS:, :] = cross
        panel[:, 0:ROWS] = cross
        b1[0:ROWS, :] = (NS_COEF_B * gram[0:ROWS, :].astype(F32) + NS_COEF_C * dot(gram[...], gram[...], 0, 0)).astype(BF16)
        swap.wait_recv()
        b1[ROWS:, :] = (NS_COEF_B * gram[ROWS:, :].astype(F32) + NS_COEF_C * dot(panel[...], gram[...], 1, 0)).astype(BF16)
        flush()
        if step == 0:
            y2p.wait_recv()
            y2m.wait_recv()
            f2 = [put(gat2.at[3, pl.ds(0, 2)], gat2.at[2, pl.ds(0, 2)], yp),
                  put(gat2.at[1, pl.ds(2, 2)], gat2.at[2, pl.ds(2, 2)], ym)]
        if not last:
            arrive = []
            for c in range(4):
                rows = pl.ds(256 * c, 256)
                upd = NS_COEF_A * cur[rows, 0:ROWS].astype(F32) + dot(cur[rows, :], b1[...], 1, 0)
                nxt[rows, 0:ROWS] = upd.astype(BF16)
                arrive.append(put(nxt.at[rows, pl.ds(0, ROWS)], nxt.at[rows, pl.ds(ROWS, ROWS)], partner))
        else:
            upd = NS_COEF_A * cur[0:64, 0:ROWS].astype(F32) + dot(cur[0:64, :], b1[...], 1, 0)
            xo1[...] = upd.astype(BF16).reshape(RING, C1, ROWS)
            back1 = [put(xo1.at[k], o1.at[z], at(k, 0, 0, 0)) for k in range(1, RING)]
            o1[z] = xo1[0]

    for copy in f2:
        copy.wait_recv()
    y2a[:, 0:ROWS] = (gat2[...].reshape(N2, ROWS).astype(F32) * inv2).astype(BF16)
    arrive2 = put(y2a.at[:, pl.ds(0, ROWS)], y2a.at[:, pl.ds(ROWS, ROWS)], partner)
    for step in range(NS_STEPS):
        last = step == NS_STEPS - 1
        cur, nxt = (y2a, y2b) if step % 2 == 0 else (y2b, y2a)
        arrive2.wait_recv()
        a2[...] = dot(cur[...], cur[...], 1, 1).astype(BF16)
        b2[...] = (NS_COEF_B * a2[...].astype(F32) + NS_COEF_C * dot(a2[...], a2[...], 1, 0)).astype(BF16)
        flush()
        if not last:
            upd = NS_COEF_A * cur[:, 0:ROWS].astype(F32) + dot(b2[...], cur[:, 0:ROWS], 1, 0)
            nxt[:, 0:ROWS] = upd.astype(BF16)
            arrive2 = put(nxt.at[:, pl.ds(0, ROWS)], nxt.at[:, pl.ds(ROWS, ROWS)], partner)
        else:
            upd = NS_COEF_A * cur[0:32, 0:ROWS].astype(F32) + dot(b2[0:32, :], cur[:, 0:ROWS], 1, 0)
            xo2[...] = upd.astype(BF16).reshape(RING, C2, ROWS)
            back2 = [put(xo2.at[k], o2.at[z], at(k, 0, 0, 0)) for k in range(1, RING)]
            o2[z] = xo2[0]

    for copy in back1:
        copy.wait_recv()
    nw1[...] = w1[...] - LEARN_RATE * (o1[...].astype(F32) * STEP_SCALE + DECAY * w1[...])
    for copy in back2:
        copy.wait_recv()
    nw2[...] = w2[...] - LEARN_RATE * (o2[...].astype(F32) * STEP_SCALE + DECAY * w2[...])
    flush()


COPIES = 160


def muon(m1, g1, m2, g2, w1, w2):
    vmem = pl.BlockSpec(memory_space=pltpu.VMEM)
    shapes = [(EXPERTS, C1, ROWS)] * 2 + [(EXPERTS, C2, ROWS)] * 2
    scratch = [
        pltpu.VMEM((EXPERTS, C1, ROWS), BF16), pltpu.VMEM((EXPERTS, C2, ROWS), BF16),
        pltpu.VMEM((EXPERTS, 2, 8, 128), F32), pltpu.VMEM((2, RING, 2, 8, 128), F32),
        pltpu.VMEM((RING, 2, 8, 128), F32), pltpu.VMEM((RING, 2, 8, 128), F32),
        pltpu.VMEM((2, 8, 128), F32), pltpu.VMEM((2, 8, 128), F32),
        pltpu.VMEM((RING, RING, RING, C1, ROWS), BF16), pltpu.VMEM((RING, RING, RING, C2, ROWS), BF16),
        pltpu.VMEM((N1, 2 * ROWS), BF16), pltpu.VMEM((N1, 2 * ROWS), BF16),
        pltpu.VMEM((2 * ROWS, ROWS), BF16), pltpu.VMEM((2 * ROWS, ROWS), BF16),
        pltpu.VMEM((ROWS, 2 * ROWS), BF16), pltpu.VMEM((ROWS, 2 * ROWS), BF16),
        pltpu.VMEM((2 * ROWS, ROWS), BF16),
        pltpu.VMEM((N2, 2 * ROWS), BF16), pltpu.VMEM((N2, 2 * ROWS), BF16),
        pltpu.VMEM((N2, N2), BF16), pltpu.VMEM((N2, N2), BF16),
        pltpu.VMEM((RING, C1, ROWS), BF16), pltpu.VMEM((RING, C2, ROWS), BF16),
        pltpu.VMEM((EXPERTS, C1, ROWS), BF16), pltpu.VMEM((EXPERTS, C2, ROWS), BF16),
        pltpu.SemaphoreType.DMA((COPIES,)), pltpu.SemaphoreType.DMA((COPIES,)),
    ]
    return pl.pallas_call(
        kernel, name='muon',
        out_shape=[jax.ShapeDtypeStruct(shape, F32) for shape in shapes],
        in_specs=[vmem] * 6, out_specs=[vmem] * 4, scratch_shapes=scratch,
        compiler_params=pltpu.CompilerParams(
            collective_id=0, has_side_effects=True, vmem_limit_bytes=56 << 20),
    )(m1, g1, m2, g2, w1, w2)


def solution(mesh):
    block_spec = P('stage', 'data', 'model')

    def local_step(w_fc1, m_fc1, g_fc1, w_fc2, m_fc2, g_fc2):
        turn = lambda arr: jnp.transpose(arr, (0, 2, 1))
        new_w1, new_m1, new_w2, new_m2 = muon(turn(m_fc1), turn(g_fc1), turn(m_fc2), turn(g_fc2), turn(w_fc1), turn(w_fc2))
        return turn(new_w1), turn(new_m1), turn(new_w2), turn(new_m2)

    return jax.shard_map(local_step, mesh=mesh, in_specs=(block_spec,) * 6, out_specs=(block_spec,) * 4, check_vma=False)
```

```python
import math
import jax
import jax.numpy as jnp
from jax import lax
from jax.experimental import pallas as pl
from jax.experimental.pallas import tpu as pltpu
from jax.sharding import PartitionSpec as P

NS_STEPS = 5
NS_COEF_A = 3.4445
NS_COEF_B = -4.7750
NS_COEF_C = 2.0315
MOMENTUM = 0.95
LEARN_RATE = 0.04
DECAY = 0.2
NORM_EPS = 1e-7
F32 = jnp.float32
BF16 = jnp.bfloat16
RING = 4
EXPERTS = 4
ROWS = 512
C1, C2 = 16, 8
N1, N2 = 1024, 512
STEP_SCALE = 0.2 * math.sqrt(1024)
CHUNKS = (256, 256, 256, 256)
NORM_Z, DATA_Z1, DATA_Z2, NORM_P, DATA_P, OUT1, OUT2, SWAP = 0, 8, 12, 16, 32, 48, 52, 56
SEMS = 160


def dot(lhs, rhs, lhs_dim, rhs_dim):
    return lax.dot_general(lhs, rhs, (((lhs_dim,), (rhs_dim,)), ((), ())), preferred_element_type=F32)


def fold(sq):
    total = None
    for row in range(0, sq.shape[0], 8):
        for col in range(0, sq.shape[1], 128):
            tile = sq[row:row + 8, col:col + 128]
            total = tile if total is None else total + tile
    return total


def flip(pos, k):
    if k == 0:
        return pos
    if k == 1:
        return pos + 1 - 2 * lax.rem(pos, 2)
    if k == 2:
        return lax.rem(pos + 2, RING)
    return RING - 1 - pos


def kernel(m1h, g1h, m2h, g2h, o1, o2,
           m1, g1, m2, g2, mb1, mb2, nb, nz, npl, sx, gat1, gat2,
           ya, yb, aa, ab, ra, rb, b1, half, y2a, y2b, a2, b2, xo1, xo2, load_sem, send_sem, recv_sem):
    idx = lax.axis_index('model')
    core = lax.axis_index('data')
    z = lax.div(idx, 16)
    y = lax.rem(lax.div(idx, 4), 4)
    x = lax.rem(idx, 4)
    mesh_id = pl.DeviceIdType.MESH

    def at(dz, dy, dx, dc):
        return {'model': flip(z, dz) * 16 + flip(y, dy) * 4 + flip(x, dx), 'data': core if dc == 0 else 1 - core}

    partner = at(0, 0, 0, 1)
    count = [0]
    swaps = [0]
    sent = []

    def put(src, dst, target, slot):
        num = count[0]
        count[0] += 1
        copy = pltpu.make_async_remote_copy(
            src_ref=src, dst_ref=dst, send_sem=send_sem.at[num], recv_sem=recv_sem.at[slot],
            device_id=target, device_id_type=mesh_id)
        copy.start()
        sent.append(copy)
        return copy

    def trade(src, dst):
        swaps[0] += 1
        return put(src, dst, partner, SWAP + swaps[0] - 1)

    def arrived(dst, slot):
        pltpu.make_async_remote_copy(
            src_ref=dst, dst_ref=dst, send_sem=send_sem.at[0], recv_sem=recv_sem.at[slot],
            device_id=partner, device_id_type=mesh_id).wait_recv()

    def flush():
        while sent:
            sent.pop(0).wait_send()

    z_peers = [(dz, dc) for dz in range(RING) for dc in range(2) if (dz, dc) != (0, 0)]
    plane = [(dy, dx) for dy in range(RING) for dx in range(RING) if (dy, dx) != (0, 0)]
    greet = [at(dz, 0, 0, dc) for dz, dc in z_peers] + [at(0, dy, dx, 0) for dy, dx in plane]
    greet += [at(dz, 0, 1, 0) for dz in range(1, RING)]
    barrier = pltpu.get_barrier_semaphore()
    for target in greet:
        pl.semaphore_signal(barrier, inc=1, device_id=target, device_id_type=mesh_id)

    loads = [pltpu.make_async_copy(src, dst, load_sem.at[i])
             for i, (src, dst) in enumerate(((m1h, m1), (g1h, g1), (m2h, m2), (g2h, g2)))]
    for copy in loads:
        copy.start()
    for copy in loads:
        copy.wait()
    for e in range(EXPERTS):
        mom = MOMENTUM * m1[e] + g1[e].astype(F32)
        mb1[e] = mom.astype(BF16)
        nb[e, 0] = fold(mom * mom)
        mom = MOMENTUM * m2[e] + g2[e].astype(F32)
        mb2[e] = mom.astype(BF16)
        nb[e, 1] = fold(mom * mom)
    pl.semaphore_wait(barrier, len(greet))

    for dz, dc in z_peers:
        put(nb.at[flip(z, dz)], nz.at[dc, dz], at(dz, 0, 0, dc), NORM_Z + 4 * dc + dz)
    for k in range(1, RING):
        put(mb1.at[flip(z, k)], gat1.at[0, k], at(k, 0, 0, 0), DATA_Z1 + k)
    for k in range(1, RING):
        put(mb2.at[flip(z, k)], gat2.at[0, k], at(k, 0, 0, 0), DATA_Z2 + k)
    gat1[0, 0] = mb1[z]
    gat2[0, 0] = mb2[z]
    part = nb[z]
    for dz, dc in z_peers:
        arrived(nz.at[dc, dz], NORM_Z + 4 * dc + dz)
        part = part + nz[dc, dz]
    sx[...] = part
    first_count, first_sent = count[0], list(sent)

    def gather(own):
        for dy, dx in plane:
            kind = (own + dy + dx) % 2
            put(sx.at[kind], npl.at[4 * dy + dx], at(0, dy, dx, 0), NORM_P + 4 * dy + dx)
        npl[0] = part[own]
        order = sorted(plane, key=lambda off: -((off[0] == 2) + (off[1] == 2) + (off[0] > 0) + (off[1] > 0)))
        for kind, gat, slot in ((0, gat1, DATA_Z1), (1, gat2, DATA_Z2)):
            for k in range(1, RING):
                arrived(gat.at[0, k], slot + k)
            for dy, dx in order:
                if (own + dy + dx) % 2 == kind:
                    put(gat.at[0], gat.at[4 * dy + dx], at(0, dy, dx, 0), DATA_P + 4 * dy + dx)

    def inverse_norm():
        total = npl[0]
        for dy, dx in plane:
            arrived(npl.at[4 * dy + dx], NORM_P + 4 * dy + dx)
            total = total + npl[4 * dy + dx]
        return 1.0 / (jnp.sqrt(jnp.sum(total, keepdims=True)) + NORM_EPS)

    def hand_out(src, dst, slot):
        keep = pltpu.make_async_copy(src.at[0, 0], dst.at[z], recv_sem.at[slot + z])
        keep.start()
        for dx in range(2):
            for dz in range(RING):
                if (dx, dz) != (0, 0):
                    put(src.at[dx, dz], dst.at[z], at(dz, 0, dx, 0), slot + z)

    own_cols, other_cols = pl.ds(0, ROWS), pl.ds(ROWS, ROWS)
    parity = lax.rem(x + y, 2)

    @pl.when(parity == 0)
    def fc1():
        gather(0)
        inv = inverse_norm()
        arrive = []
        for c in range(4):
            for s in range(4 * c, 4 * c + 4):
                if s:
                    arrived(gat1.at[s], DATA_P + s)
            rows = pl.ds(256 * c, 256)
            ya[rows, own_cols] = (gat1[4 * c:4 * c + 4].reshape(256, ROWS).astype(F32) * inv).astype(BF16)
            arrive.append(trade(ya.at[rows, own_cols], ya.at[rows, other_cols]))
        for step in range(NS_STEPS):
            cur, nxt = (ya, yb) if step % 2 == 0 else (yb, ya)
            gram, panel = (aa, ra) if step % 2 == 0 else (ab, rb)
            gram[0:ROWS, :] = dot(cur[:, 0:ROWS], cur[:, 0:ROWS], 0, 0).astype(BF16)
            swap = trade(gram.at[pl.ds(0, ROWS)], panel.at[:, other_cols])
            half[...] = dot(gram[0:ROWS, :], gram[0:ROWS, :], 1, 0)
            for copy in arrive:
                copy.wait_recv()
            cross = dot(cur[:, ROWS:], cur[:, 0:ROWS], 0, 0).astype(BF16)
            gram[ROWS:, :] = cross
            panel[:, 0:ROWS] = cross
            square = half[...] + dot(gram[ROWS:, :], gram[ROWS:, :], 0, 0)
            b1[0:ROWS, :] = (NS_COEF_B * gram[0:ROWS, :].astype(F32) + NS_COEF_C * square).astype(BF16)
            swap.wait_recv()
            square = dot(panel[...], gram[...], 1, 0)
            b1[ROWS:, :] = (NS_COEF_B * gram[ROWS:, :].astype(F32) + NS_COEF_C * square).astype(BF16)
            flush()
            if step < NS_STEPS - 1:
                arrive = []
                base = 0
                for size in CHUNKS:
                    rows = pl.ds(base, size)
                    upd = NS_COEF_A * cur[rows, 0:ROWS].astype(F32) + dot(cur[rows, :], b1[...], 1, 0)
                    nxt[rows, 0:ROWS] = upd.astype(BF16)
                    arrive.append(trade(nxt.at[rows, own_cols], nxt.at[rows, other_cols]))
                    base += size
            else:
                upd = NS_COEF_A * cur[0:128, 0:ROWS].astype(F32) + dot(cur[0:128, :], b1[...], 1, 0)
                xo1[...] = upd.astype(BF16).reshape(2, RING, C1, ROWS)
                hand_out(xo1, o1, OUT1)
        flush()

    count[0] = first_count
    swaps[0] = 0
    sent[:] = first_sent

    @pl.when(parity == 1)
    def fc2():
        gather(1)
        inv = inverse_norm()
        for s in range(1, 16):
            arrived(gat2.at[s], DATA_P + s)
        y2a[:, 0:ROWS] = (gat2[...].reshape(N2, ROWS).astype(F32) * inv).astype(BF16)
        arrive = trade(y2a.at[:, own_cols], y2a.at[:, other_cols])
        for step in range(NS_STEPS):
            cur, nxt = (y2a, y2b) if step % 2 == 0 else (y2b, y2a)
            arrive.wait_recv()
            a2[...] = dot(cur[...], cur[...], 1, 1).astype(BF16)
            b2[...] = (NS_COEF_B * a2[...].astype(F32) + NS_COEF_C * dot(a2[...], a2[...], 1, 0)).astype(BF16)
            flush()
            if step < NS_STEPS - 1:
                upd = NS_COEF_A * cur[:, 0:ROWS].astype(F32) + dot(b2[...], cur[:, 0:ROWS], 1, 0)
                nxt[:, 0:ROWS] = upd.astype(BF16)
                arrive = trade(nxt.at[:, own_cols], nxt.at[:, other_cols])
            else:
                upd = NS_COEF_A * cur[0:64, 0:ROWS].astype(F32) + dot(b2[0:64, :], cur[:, 0:ROWS], 1, 0)
                xo2[...] = upd.astype(BF16).reshape(2, RING, C2, ROWS)
                hand_out(xo2, o2, OUT2)
        flush()

    for e in range(EXPERTS):
        arrived(o2.at[e], OUT2 + e)
        arrived(o1.at[e], OUT1 + e)


def muon(m1, g1, m2, g2):
    vmem = pl.BlockSpec(memory_space=pltpu.VMEM)
    hbm = pl.BlockSpec(memory_space=pltpu.HBM)
    big, small = (EXPERTS, C1, ROWS), (EXPERTS, C2, ROWS)
    scratch = [
        pltpu.VMEM(big, F32), pltpu.VMEM(big, BF16), pltpu.VMEM(small, F32), pltpu.VMEM(small, BF16),
        pltpu.VMEM(big, BF16), pltpu.VMEM(small, BF16),
        pltpu.VMEM((EXPERTS, 2, 8, 128), F32), pltpu.VMEM((2, RING, 2, 8, 128), F32),
        pltpu.VMEM((16, 8, 128), F32), pltpu.VMEM((2, 8, 128), F32),
        pltpu.VMEM((16, RING, C1, ROWS), BF16), pltpu.VMEM((16, RING, C2, ROWS), BF16),
        pltpu.VMEM((N1, 2 * ROWS), BF16), pltpu.VMEM((N1, 2 * ROWS), BF16),
        pltpu.VMEM((2 * ROWS, ROWS), BF16), pltpu.VMEM((2 * ROWS, ROWS), BF16),
        pltpu.VMEM((ROWS, 2 * ROWS), BF16), pltpu.VMEM((ROWS, 2 * ROWS), BF16),
        pltpu.VMEM((2 * ROWS, ROWS), BF16), pltpu.VMEM((ROWS, ROWS), F32),
        pltpu.VMEM((N2, 2 * ROWS), BF16), pltpu.VMEM((N2, 2 * ROWS), BF16),
        pltpu.VMEM((N2, N2), BF16), pltpu.VMEM((N2, N2), BF16),
        pltpu.VMEM((2, RING, C1, ROWS), BF16), pltpu.VMEM((2, RING, C2, ROWS), BF16),
        pltpu.SemaphoreType.DMA((4,)), pltpu.SemaphoreType.DMA((SEMS,)), pltpu.SemaphoreType.DMA((SEMS,)),
    ]
    return pl.pallas_call(
        kernel, name='muon',
        out_shape=[jax.ShapeDtypeStruct(big, BF16), jax.ShapeDtypeStruct(small, BF16)],
        in_specs=[hbm] * 4, out_specs=[vmem] * 2, scratch_shapes=scratch,
        cost_estimate=pl.CostEstimate(flops=16_000_000_000, bytes_accessed=1 << 20, transcendentals=0),
        compiler_params=pltpu.CompilerParams(
            collective_id=0, has_side_effects=True, vmem_limit_bytes=63 << 20),
    )(m1, g1, m2, g2)


def solution(mesh):
    block_spec = P('stage', 'data', 'model')

    def local_step(w_fc1, m_fc1, g_fc1, w_fc2, m_fc2, g_fc2):
        turn = lambda arr: jnp.transpose(arr, (0, 2, 1))
        o_fc1, o_fc2 = muon(turn(m_fc1), turn(g_fc1), turn(m_fc2), turn(g_fc2))
        outs = []
        for w, m, g, o in ((w_fc1, m_fc1, g_fc1, o_fc1), (w_fc2, m_fc2, g_fc2, o_fc2)):
            step = turn(o).astype(F32) * STEP_SCALE
            outs += [w - LEARN_RATE * (step + DECAY * w), MOMENTUM * m + g.astype(F32)]
        return tuple(outs)

    return jax.shard_map(local_step, mesh=mesh, in_specs=(block_spec,) * 6, out_specs=(block_spec,) * 4, check_vma=False)
```

```python
import math
import jax
import jax.numpy as jnp
from jax import lax
from jax.experimental import pallas as pl
from jax.experimental.pallas import tpu as pltpu
from jax.sharding import PartitionSpec as P

NS_STEPS = 5
NS_COEF_A = 3.4445
NS_COEF_B = -4.7750
NS_COEF_C = 2.0315
MOMENTUM = 0.95
LEARN_RATE = 0.04
DECAY = 0.2
NORM_EPS = 1e-7
F32 = jnp.float32
BF16 = jnp.bfloat16
RING = 4
EXPERTS = 4
ROWS = 512
C1, C2 = 16, 8
N1, N2 = 1024, 512
STEP_SCALE = 0.2 * math.sqrt(1024)
CHUNKS = (384, 384, 256)
ARRIVAL = (0, 1, 3, 2)
NORM_Z, DATA_Z1, DATA_Z2, NORM_P, DATA_P, OUT1, OUT2, SWAP = 0, 8, 12, 16, 32, 48, 52, 56
SEMS = 160


def dot(lhs, rhs, lhs_dim, rhs_dim):
    return lax.dot_general(lhs, rhs, (((lhs_dim,), (rhs_dim,)), ((), ())), preferred_element_type=F32)


def fold(sq):
    total = None
    for row in range(0, sq.shape[0], 8):
        for col in range(0, sq.shape[1], 128):
            tile = sq[row:row + 8, col:col + 128]
            total = tile if total is None else total + tile
    return total


def flip(pos, k):
    if k == 0:
        return pos
    if k == 1:
        return pos + 1 - 2 * lax.rem(pos, 2)
    if k == 2:
        return lax.rem(pos + 2, RING)
    return RING - 1 - pos


def kernel(m1h, g1h, m2h, g2h, o1, o2,
           m1, g1, m2, g2, mb1, mb2, nb, nz, npl, sx, total, gat1, gat2,
           ya, yb, aa, ab, ra, rb, b1, half, acc, y2a, y2b, a2, b2, xo1, xo2, load_sem, send_sem, recv_sem):
    idx = lax.axis_index('model')
    core = lax.axis_index('data')
    z = lax.div(idx, 16)
    y = lax.rem(lax.div(idx, 4), 4)
    x = lax.rem(idx, 4)
    mesh_id = pl.DeviceIdType.MESH

    def at(dz, dy, dx, dc):
        return {'model': flip(z, dz) * 16 + flip(y, dy) * 4 + flip(x, dx), 'data': core if dc == 0 else 1 - core}

    partner = at(0, 0, 0, 1)
    count = [0]
    swaps = [0]
    sent = []

    def put(src, dst, target, slot):
        num = count[0]
        count[0] += 1
        copy = pltpu.make_async_remote_copy(
            src_ref=src, dst_ref=dst, send_sem=send_sem.at[num], recv_sem=recv_sem.at[slot],
            device_id=target, device_id_type=mesh_id)
        copy.start()
        sent.append(copy)
        return copy

    def trade(src, dst):
        swaps[0] += 1
        return put(src, dst, partner, SWAP + swaps[0] - 1)

    def arrived(dst, slot):
        pltpu.make_async_remote_copy(
            src_ref=dst, dst_ref=dst, send_sem=send_sem.at[0], recv_sem=recv_sem.at[slot],
            device_id=partner, device_id_type=mesh_id).wait_recv()

    def flush():
        while sent:
            sent.pop(0).wait_send()

    z_peers = [(dz, dc) for dz in range(RING) for dc in range(2) if (dz, dc) != (0, 0)]
    plane = [(dy, dx) for dy in range(RING) for dx in range(RING) if (dy, dx) != (0, 0)]
    greet = [at(dz, 0, 0, dc) for dz, dc in z_peers] + [at(0, dy, dx, 0) for dy, dx in plane]
    greet += [at(dz, 0, 1, 0) for dz in range(1, RING)]
    barrier = pltpu.get_barrier_semaphore()
    for target in greet:
        pl.semaphore_signal(barrier, inc=1, device_id=target, device_id_type=mesh_id)

    loads = [pltpu.make_async_copy(src, dst, load_sem.at[i])
             for i, (src, dst) in enumerate(((m1h, m1), (g1h, g1), (m2h, m2), (g2h, g2)))]
    for copy in loads:
        copy.start()
    for copy in loads:
        copy.wait()
    nb[...] = jnp.zeros_like(nb)
    for e in range(EXPERTS):
        mom = MOMENTUM * m1[e] + g1[e].astype(F32)
        mb1[e] = mom.astype(BF16)
        nb[0, e:e + 1] = jnp.sum(fold(mom * mom), axis=0, keepdims=True)
        mom = MOMENTUM * m2[e] + g2[e].astype(F32)
        mb2[e] = mom.astype(BF16)
        nb[1, e:e + 1] = jnp.sum(fold(mom * mom), axis=0, keepdims=True)
    gat1[0, 0] = mb1[z]
    gat2[0, 0] = mb2[z]
    pl.semaphore_wait(barrier, len(greet))

    for k in (2, 1, 3):
        put(mb1.at[flip(z, k)], gat1.at[0, k], at(k, 0, 0, 0), DATA_Z1 + k)
    for k in range(1, RING):
        put(mb2.at[flip(z, k)], gat2.at[0, k], at(k, 0, 0, 0), DATA_Z2 + k)
    first_count, first_sent = count[0], list(sent)

    def gather(own):
        order = sorted(plane, key=lambda off: -((off[0] == 2) + (off[1] == 2) + (off[0] > 0) + (off[1] > 0)))
        for dy, dx in order:
            kind = (own + dy + dx) % 2
            put(nb.at[kind], npl.at[4 * dy + dx], at(0, dy, dx, 0), NORM_P + 4 * dy + dx)
        for k in (0, 1, 3, 2):
            if k:
                arrived(gat1.at[0, k], DATA_Z1 + k)
            for dy, dx in order:
                if (own + dy + dx) % 2 == 0:
                    put(gat1.at[0, k], gat1.at[4 * dy + dx, k], at(0, dy, dx, 0), DATA_P + 4 * dy + dx)
        part = nb[own]
        for dy, dx in plane:
            arrived(npl.at[4 * dy + dx], NORM_P + 4 * dy + dx)
            part = part + npl[4 * dy + dx]
        sx[...] = part
        for dz, dc in z_peers:
            put(sx, nz.at[4 * dc + dz], at(dz, 0, 0, dc), NORM_Z + 4 * dc + dz)
        for k in range(1, RING):
            arrived(gat2.at[0, k], DATA_Z2 + k)
        for dy, dx in order:
            if (own + dy + dx) % 2 == 1:
                put(gat2.at[0], gat2.at[4 * dy + dx], at(0, dy, dx, 0), DATA_P + 4 * dy + dx)
        for dz, dc in z_peers:
            arrived(nz.at[4 * dc + dz], NORM_Z + 4 * dc + dz)
            part = part + nz[4 * dc + dz]
        total[...] = part
        return 1.0 / (jnp.sqrt(jnp.sum(total[pl.ds(z, 1), :], keepdims=True)) + NORM_EPS)

    def hand_out(src, dst, slot):
        keep = pltpu.make_async_copy(src.at[0, 0], dst.at[z], recv_sem.at[slot + z])
        keep.start()
        for dx in (1, 0):
            for dz in (2, 1, 3, 0):
                if (dx, dz) != (0, 0):
                    put(src.at[dx, dz], dst.at[z], at(dz, 0, dx, 0), slot + z)

    own_cols, other_cols = pl.ds(0, ROWS), pl.ds(ROWS, ROWS)
    parity = lax.rem(x + y, 2)

    @pl.when(parity == 0)
    def fc1():
        inv = gather(0)
        arrive = []
        for i, c in enumerate(ARRIVAL):
            for s in range(4 * c, 4 * c + 4):
                if s:
                    arrived(gat1.at[s], DATA_P + s)
            rows = pl.ds(256 * c, 256)
            ya[rows, own_cols] = (gat1[4 * c:4 * c + 4].reshape(256, ROWS).astype(F32) * inv).astype(BF16)
            arrive.append(trade(ya.at[rows, own_cols], ya.at[rows, other_cols]))
            piece = dot(ya[rows, 0:ROWS], ya[rows, 0:ROWS], 0, 0)
            half[...] = piece if i == 0 else half[...] + piece
            if i:
                rows = pl.ds(256 * ARRIVAL[i - 1], 256)
                arrive[i - 1].wait_recv()
                piece = dot(ya[rows, ROWS:], ya[rows, 0:ROWS], 0, 0)
                acc[...] = piece if i == 1 else acc[...] + piece
        arrive = arrive[-1:]
        for step in range(NS_STEPS):
            cur, nxt = (ya, yb) if step % 2 == 0 else (yb, ya)
            gram, far = (aa, ra) if step % 2 == 0 else (ab, rb)
            near = half[...] if step == 0 else dot(cur[:, 0:ROWS], cur[:, 0:ROWS], 0, 0)
            gram[0:ROWS, :] = near.astype(BF16)
            swap = trade(gram.at[pl.ds(0, ROWS)], far)
            half[...] = dot(gram[0:ROWS, :], gram[0:ROWS, :], 1, 0)
            for copy in arrive:
                copy.wait_recv()
            if step == 0:
                rows = pl.ds(256 * ARRIVAL[-1], 256)
                cross = acc[...] + dot(cur[rows, ROWS:], cur[rows, 0:ROWS], 0, 0)
            else:
                cross = dot(cur[:, ROWS:], cur[:, 0:ROWS], 0, 0)
            gram[ROWS:, :] = cross.astype(BF16)
            square = half[...] + dot(gram[ROWS:, :], gram[ROWS:, :], 0, 0)
            b1[0:ROWS, :] = (NS_COEF_B * gram[0:ROWS, :].astype(F32) + NS_COEF_C * square).astype(BF16)
            acc[...] = dot(gram[ROWS:, :], gram[0:ROWS, :], 1, 0)
            swap.wait_recv()
            flush()
            square = acc[...] + dot(far[...], gram[ROWS:, :], 1, 0)
            b1[ROWS:, :] = (NS_COEF_B * gram[ROWS:, :].astype(F32) + NS_COEF_C * square).astype(BF16)
            if step < NS_STEPS - 1:
                arrive = []
                base = 0
                for size in CHUNKS:
                    rows = pl.ds(base, size)
                    upd = NS_COEF_A * cur[rows, 0:ROWS].astype(F32) + dot(cur[rows, :], b1[...], 1, 0)
                    nxt[rows, 0:ROWS] = upd.astype(BF16)
                    arrive.append(trade(nxt.at[rows, own_cols], nxt.at[rows, other_cols]))
                    base += size
            else:
                upd = NS_COEF_A * cur[0:128, 0:ROWS].astype(F32) + dot(cur[0:128, :], b1[...], 1, 0)
                xo1[...] = upd.astype(BF16).reshape(2, RING, C1, ROWS)
                hand_out(xo1, o1, OUT1)
        flush()

    count[0] = first_count
    swaps[0] = 0
    sent[:] = first_sent

    @pl.when(parity == 1)
    def fc2():
        inv = gather(1)
        for s in range(1, 16):
            arrived(gat2.at[s], DATA_P + s)
        y2a[:, 0:ROWS] = (gat2[...].reshape(N2, ROWS).astype(F32) * inv).astype(BF16)
        arrive = trade(y2a.at[:, own_cols], y2a.at[:, other_cols])
        for step in range(NS_STEPS):
            cur, nxt = (y2a, y2b) if step % 2 == 0 else (y2b, y2a)
            arrive.wait_recv()
            a2[...] = dot(cur[...], cur[...], 1, 1).astype(BF16)
            b2[...] = (NS_COEF_B * a2[...].astype(F32) + NS_COEF_C * dot(a2[...], a2[...], 1, 0)).astype(BF16)
            flush()
            if step < NS_STEPS - 1:
                upd = NS_COEF_A * cur[:, 0:ROWS].astype(F32) + dot(b2[...], cur[:, 0:ROWS], 1, 0)
                nxt[:, 0:ROWS] = upd.astype(BF16)
                arrive = trade(nxt.at[:, own_cols], nxt.at[:, other_cols])
            else:
                upd = NS_COEF_A * cur[0:64, 0:ROWS].astype(F32) + dot(b2[0:64, :], cur[:, 0:ROWS], 1, 0)
                xo2[...] = upd.astype(BF16).reshape(2, RING, C2, ROWS)
                hand_out(xo2, o2, OUT2)
        flush()

    for e in range(EXPERTS):
        arrived(o2.at[e], OUT2 + e)
        arrived(o1.at[e], OUT1 + e)


def muon(m1, g1, m2, g2):
    vmem = pl.BlockSpec(memory_space=pltpu.VMEM)
    hbm = pl.BlockSpec(memory_space=pltpu.HBM)
    big, small = (EXPERTS, C1, ROWS), (EXPERTS, C2, ROWS)
    scratch = [
        pltpu.VMEM(big, F32), pltpu.VMEM(big, BF16), pltpu.VMEM(small, F32), pltpu.VMEM(small, BF16),
        pltpu.VMEM(big, BF16), pltpu.VMEM(small, BF16),
        pltpu.VMEM((2, 8, 128), F32), pltpu.VMEM((2 * RING, 8, 128), F32), pltpu.VMEM((16, 8, 128), F32),
        pltpu.VMEM((8, 128), F32), pltpu.VMEM((8, 128), F32),
        pltpu.VMEM((16, RING, C1, ROWS), BF16), pltpu.VMEM((16, RING, C2, ROWS), BF16),
        pltpu.VMEM((N1, 2 * ROWS), BF16), pltpu.VMEM((N1, 2 * ROWS), BF16),
        pltpu.VMEM((2 * ROWS, ROWS), BF16), pltpu.VMEM((2 * ROWS, ROWS), BF16),
        pltpu.VMEM((ROWS, ROWS), BF16), pltpu.VMEM((ROWS, ROWS), BF16),
        pltpu.VMEM((2 * ROWS, ROWS), BF16), pltpu.VMEM((ROWS, ROWS), F32), pltpu.VMEM((ROWS, ROWS), F32),
        pltpu.VMEM((N2, 2 * ROWS), BF16), pltpu.VMEM((N2, 2 * ROWS), BF16),
        pltpu.VMEM((N2, N2), BF16), pltpu.VMEM((N2, N2), BF16),
        pltpu.VMEM((2, RING, C1, ROWS), BF16), pltpu.VMEM((2, RING, C2, ROWS), BF16),
        pltpu.SemaphoreType.DMA((4,)), pltpu.SemaphoreType.DMA((SEMS,)), pltpu.SemaphoreType.DMA((SEMS,)),
    ]
    return pl.pallas_call(
        kernel, name='muon',
        out_shape=[jax.ShapeDtypeStruct(big, BF16), jax.ShapeDtypeStruct(small, BF16)],
        in_specs=[hbm] * 4, out_specs=[vmem] * 2, scratch_shapes=scratch,
        cost_estimate=pl.CostEstimate(flops=16_000_000_000, bytes_accessed=1 << 20, transcendentals=0),
        compiler_params=pltpu.CompilerParams(
            collective_id=0, has_side_effects=True, vmem_limit_bytes=40 << 20),
    )(*[pltpu.with_memory_space_constraint(arg, pltpu.HBM) for arg in (m1, g1, m2, g2)])


def solution(mesh):
    block_spec = P('stage', 'data', 'model')

    def local_step(w_fc1, m_fc1, g_fc1, w_fc2, m_fc2, g_fc2):
        turn = lambda arr: jnp.transpose(arr, (0, 2, 1))
        o_fc1, o_fc2 = muon(turn(m_fc1), turn(g_fc1), turn(m_fc2), turn(g_fc2))
        outs = []
        for w, m, g, o in ((w_fc1, m_fc1, g_fc1, o_fc1), (w_fc2, m_fc2, g_fc2, o_fc2)):
            step = turn(o).astype(F32) * STEP_SCALE
            outs += [w - LEARN_RATE * (step + DECAY * w), MOMENTUM * m + g.astype(F32)]
        return tuple(outs)

    return jax.shard_map(local_step, mesh=mesh, in_specs=(block_spec,) * 6, out_specs=(block_spec,) * 4, check_vma=False)
```
